128 devices in a mesh: aa: 32 (over y, z_hi, x), ba: 4 (over z_lo, core).
Axes of the slice: x: 4, y: 4, z: 4 (z_hi: 2, z_lo: 2; z = z_hi * 2 + z_lo), core: 2. Of those that a mesh axis runs over, the one named last changes fastest.
Arguments:
- fast_query: bfloat16 [2, 8192, 5120], P(None, 'aa', 'ba'), may hold values from -6 to 6
- fast_key: bfloat16 [2, 8192, 5120], P(None, 'aa', 'ba'), may hold values from -6 to 6
- fast_value: bfloat16 [2, 8192, 5120], P(None, 'aa', 'ba'), may hold values from -6 to 6
- rates: float32 [2, 8192, 24], P(None, 'aa', 'ba'), may hold values from 5e-05 to 0.0005
- attn_query: bfloat16 [2, 8192, 5120], P(None, 'aa', 'ba'), may hold values from -4.5 to 4.5
- attn_key: bfloat16 [2, 8192, 5120], P(None, 'aa', 'ba'), may hold values from -4.5 to 4.5
- attn_value: bfloat16 [2, 8192, 5120], P(None, 'aa', 'ba'), may hold values from -6 to 6
- fast_weights: float32 [640, 3, 8, 640], P('aa', None, 'ba'), may hold values from -0.2814427 to 0.2814427
- gain: float32 [5120], replicated, may hold values from 0.5 to 1.5
Outputs:
- mixed: bfloat16 [2, 8192, 5120], P(None, ('aa', 'ba'))
- weights_out: float32 [640, 3, 8, 640], P('aa', None, 'ba')
- moment_out: float32 [640, 3, 8, 640], P('aa', None, 'ba')
The draws below stay inside these ranges and needn't reach their ends.
All inputs are finite; a program needn't handle non-finite values.
Results may differ from the reference program's by a relative error of at most 0.028.
Values may be sent and summed in bfloat16 or wider, within the bound.
No kernel may reach another device: no remote copies, remote signals or barrier semaphores. Data moves between devices by JAX's collectives and lax.ppermute only.
A program may use at most 192 MiB of HBM per device.

```python
import math
import jax
import jax.numpy as jnp
from jax import lax

H = 8
DH = 640
FH = 640
AH = 40
AD = 128
WINDOW = 512
STRETCHES = 2
TOK_DEV = 256
TOKENS = 8192
N_AA = 32


def attention_pair(key):
    base = jax.random.fold_in(key, 7)
    key_q, key_k = jax.random.split(base, 2)
    shape = (STRETCHES, TOKENS, AH * AD)
    query = jnp.clip(jax.random.normal(key_q, shape, jnp.float32), -4.5, 4.5)
    keys = jnp.clip(jax.random.normal(key_k, shape, jnp.float32), -4.5, 4.5)
    return (query, keys)


def draw_attn_query(key, part):
    query, keys = attention_pair(key)
    return query.astype(jnp.bfloat16)


def draw_attn_key(key, part):
    query, keys = attention_pair(key)
    return keys.astype(jnp.bfloat16)


def draw_fast_weights(key, part):
    key_b, key_c = jax.random.split(jax.random.fold_in(key, 11), 2)
    shape = (FH, 3, H, DH)
    base = jnp.clip(jax.random.normal(key_b, shape, jnp.float32), -4.0, 4.0)
    cols = jnp.exp(jax.random.uniform(key_c, (3, H, DH), jnp.float32, 0.0, math.log(10.0)))
    return base * cols[None] * (8.0 / (45.0 * math.sqrt(DH)))


def levels(rng, shape, shards, least, top_value):
    factor_of = 1.0
    for position, parts in shards:
        steps = jax.random.uniform(jax.random.fold_in(jax.random.fold_in(rng, 6), position), (parts,), jnp.float32, least / len(shards), top_value / len(shards))
        factor_of = factor_of * jnp.repeat(jnp.exp(steps), shape[position] // parts).reshape((-1,) + (1,) * (len(shape) - 1 - position))
    return factor_of


def bell_draw(key, dims, scale, most, shards=(), held_as=jnp.bfloat16):
    values = scale * jax.random.normal(key, dims, jnp.float32)
    if shards:
        values = values * levels(key, dims, shards, -0.22, 0.18)
    return jnp.clip(values, -most, most).astype(held_as)


def setup_inputs(seed: int = 0) -> dict:
    splits = jax.random.split(jax.random.key(seed), 10)
    fast_query = bell_draw(splits[0], (STRETCHES, TOKENS, H * DH), 1.0, 6.0, ((1, 32), (2, 4)))
    fast_key = bell_draw(splits[1], (STRETCHES, TOKENS, H * DH), 1.0, 6.0, ((1, 32), (2, 4)))
    fast_value = bell_draw(splits[2], (STRETCHES, TOKENS, H * DH), 1.0, 6.0, ((1, 32), (2, 4)))
    rates = jnp.clip(jnp.exp(math.log(0.0005) - 2.3025852 * jax.random.uniform(splits[3], (STRETCHES, TOKENS, 3 * H), jnp.float32) ** levels(splits[3], (STRETCHES, TOKENS, 3 * H), ((1, 32), (2, 4)), -0.2, 0.2)), 4.999999873689376e-05, 0.0005)
    attn_query = draw_attn_query(jax.random.fold_in(splits[9], 71), 0)
    attn_key = draw_attn_key(jax.random.fold_in(splits[9], 71), 0)
    attn_value = bell_draw(splits[6], (STRETCHES, TOKENS, AH * AD), 1.0, 6.0, ((1, 32), (2, 4)))
    fast_weights = draw_fast_weights(jax.random.fold_in(splits[9], 71), 0)
    gain = jnp.clip(1.0 + 0.1 * jax.random.normal(splits[8], (H * DH,), jnp.float32), 0.5, 1.5)
    return {"fast_query": fast_query, "fast_key": fast_key, "fast_value": fast_value, "rates": rates, "attn_query": attn_query, "attn_key": attn_key, "attn_value": attn_value, "fast_weights": fast_weights, "gain": gain}


BETA = 0.9
EPS = 1e-06

def activation(x):
    sig = jax.nn.sigmoid(x)
    return (x * sig, sig * (1.0 + x * (1.0 - sig)))

def project(x, w):
    return jnp.einsum('nhd,fhd->nhf', x.astype(jnp.float32), w.astype(jnp.float32))

def fast_stretch(weights, query, key, value, rate):
    tokens = query.shape[0]
    wbf = weights.astype(jnp.bfloat16)
    q = query.reshape(tokens, H, DH)
    k = key.reshape(tokens, H, DH)
    v = value.reshape(tokens, H, DH)
    act_q, slope_q = activation(project(q, wbf[:, 0]))
    hidden_q = (act_q * project(q, wbf[:, 1])).astype(jnp.bfloat16)
    out = jnp.einsum('nhf,fhd->nhd', hidden_q.astype(jnp.float32), wbf[:, 2].astype(jnp.float32)).reshape(tokens, H * DH)
    gate_in = project(k, wbf[:, 0])
    up_in = project(k, wbf[:, 1])
    back_in = project(v, wbf[:, 2])
    act, slope = activation(gate_in)
    rate = rate.reshape(tokens, H, 3)
    gate_x = (rate[..., 0:1] * (-back_in * up_in * slope)).astype(jnp.bfloat16)
    up_x = (rate[..., 1:2] * (-back_in * act)).astype(jnp.bfloat16)
    down_x = (rate[..., 2:3] * -(act * up_in)).astype(jnp.bfloat16)

    def block(total, index):
        start = index * TOK_DEV

        def cut(x):
            return lax.dynamic_slice_in_dim(x, start, TOK_DEV, 0).astype(jnp.float32)
        gate_g = jnp.einsum('nhf,nhd->fhd', cut(gate_x), cut(k))
        up_g = jnp.einsum('nhf,nhd->fhd', cut(up_x), cut(k))
        down_g = jnp.einsum('nhf,nhd->fhd', cut(down_x), cut(v))
        stacked = jnp.stack([gate_g, up_g, down_g], 1)
        rounded = lax.optimization_barrier(stacked.astype(jnp.bfloat16))
        return (total + rounded.astype(jnp.float32), None)
    grads, unused = lax.scan(block, jnp.zeros((FH, 3, H, DH), jnp.float32), jnp.arange(N_AA, dtype=jnp.int32))
    return (out, grads)

def renorm(trial, target):
    return trial * (target / jnp.sqrt(lax.optimization_barrier(jnp.sum(trial * trial, 0)) + EPS))

def attend(query, key, value):
    total = STRETCHES * TOKENS
    q = query.reshape(total, AH, AD)
    k = key.reshape(total, AH, AD)
    v = value.reshape(total, AH, AD)
    reach = (WINDOW - 2) // TOK_DEV + 1
    margin = reach * TOK_DEV
    k_pad = jnp.concatenate([jnp.zeros((margin, AH, AD), k.dtype), k], 0)
    v_pad = jnp.concatenate([jnp.zeros((margin, AH, AD), v.dtype), v], 0)

    def block(index):
        start = index * TOK_DEV
        q_blk = lax.dynamic_slice_in_dim(q, start, TOK_DEV, 0).astype(jnp.float32)
        k_blk = lax.dynamic_slice_in_dim(k_pad, start, margin + TOK_DEV, 0).astype(jnp.float32)
        v_blk = lax.dynamic_slice_in_dim(v_pad, start, margin + TOK_DEV, 0).astype(jnp.float32)
        scores = jnp.einsum('qhe,khe->hqk', q_blk, k_blk) / math.sqrt(AD)
        q_pos = start + jnp.arange(TOK_DEV, dtype=jnp.int32)
        k_pos = start - margin + jnp.arange(margin + TOK_DEV, dtype=jnp.int32)
        mask = (k_pos[None, :] <= q_pos[:, None]) & (k_pos[None, :] > q_pos[:, None] - WINDOW) & (k_pos[None, :] >= 0)
        scores = jnp.where(mask[None], scores, -1e+30)
        top = lax.optimization_barrier(jnp.max(scores, -1, keepdims=True))
        probs = jnp.exp(scores - top)
        denom = lax.optimization_barrier(jnp.sum(probs, -1))
        rounded = lax.optimization_barrier(probs.astype(jnp.bfloat16)).astype(jnp.float32)
        out = jnp.einsum('hqk,khe->qhe', rounded, v_blk)
        return out / jnp.transpose(denom)[:, :, None]
    outs = lax.map(block, jnp.arange(total // TOK_DEV, dtype=jnp.int32))
    return outs.reshape(STRETCHES, TOKENS, AH * AD)

def reference(fast_query, fast_key, fast_value, rates, attn_query, attn_key, attn_value, fast_weights, gain):
    target = jnp.sqrt(lax.optimization_barrier(jnp.sum(fast_weights * fast_weights, 0)) + EPS)
    weights = fast_weights
    moment = jnp.zeros_like(fast_weights)
    fast_out = []
    for stretch in range(STRETCHES):
        out, grads = fast_stretch(weights, fast_query[stretch], fast_key[stretch], fast_value[stretch], rates[stretch])
        fast_out.append(out)
        moment = BETA * moment + grads
        weights = renorm(weights - moment, target)
    attention = attend(attn_query, attn_key, attn_value)
    combined = lax.optimization_barrier((jnp.stack(fast_out) + attention).astype(jnp.bfloat16)).astype(jnp.float32)
    scale = lax.rsqrt(lax.optimization_barrier(jnp.mean(combined * combined, -1, keepdims=True)) + EPS)
    mixed = (combined * scale * gain).astype(jnp.bfloat16)
    return (mixed, weights, moment)
```

```python
import math

import jax
import jax.numpy as jnp
from jax import lax
from jax.experimental import pallas as pl
from jax.experimental.pallas import tpu as pltpu
from jax.sharding import Mesh
from jax.sharding import PartitionSpec as P

AD = 128
WINDOW = 512
AA = ("aa_0", "aa_1", "aa_2")
BA = ("ba_0", "ba_1")
AA_BA = ("aa_0", "aa_1", "aa_2", "ba_0", "ba_1")
PLANE = ("aa_0", "aa_2")
PAIR = "aa_1"

BETA = 0.9
EPS = 1e-06


def activation(x):
    sig = jax.nn.sigmoid(x)
    return (x * sig, sig * (1.0 + x * (1.0 - sig)))


def partner(x):
    return lax.ppermute(x, PAIR, [(0, 1), (1, 0)])


def sent_to_all(shard, axis):
    copies = jnp.broadcast_to(shard, (lax.axis_size(axis), *shard.shape))
    return lax.all_to_all(copies, axis, split_axis=0, concat_axis=0, tiled=True)


def from_behind(shard, axis, by):
    length = lax.axis_size(axis)
    return lax.ppermute(shard, axis, [(i, (i + by) % length) for i in range(length)])


def times_t(x, w):
    return lax.dot_general(x, w, (((1,), (1,)), ((), ())), preferred_element_type=jnp.float32)


def t_times(x, y):
    return lax.dot_general(x, y, (((0,), (0,)), ((), ())), preferred_element_type=jnp.float32)


def matrices(full):
    depth = full.shape[-1]
    return [full[:, i].reshape(-1, depth) for i in range(3)]


def answers(gate, up, down, q):
    act, _ = activation(times_t(q, gate))
    hidden = (act * times_t(q, up)).astype(jnp.bfloat16)
    return jnp.dot(hidden, down, preferred_element_type=jnp.float32)


def gradient(gate, up, down, k, v, rate, parts):
    gate_in = times_t(k, gate)
    up_in = times_t(k, up)
    back_in = times_t(v, down)
    act, slope = activation(gate_in)
    gate_x = (rate[:, 0:1] * (-back_in * up_in * slope)).astype(jnp.bfloat16)
    up_x = (rate[:, 1:2] * (-back_in * act)).astype(jnp.bfloat16)
    down_x = (rate[:, 2:3] * -(act * up_in)).astype(jnp.bfloat16)
    terms = [t_times(gate_x, k), t_times(up_x, k), t_times(down_x, v)]
    return jnp.stack(
        [t.astype(jnp.bfloat16).reshape(parts, -1, t.shape[-1]) for t in terms], 1
    )


def summed_rows(terms):
    got = lax.all_to_all(terms, PLANE, split_axis=0, concat_axis=0, tiled=True)
    return jnp.sum(got.astype(jnp.float32), 0)


def attend_kernel(early_ref, q_ref, k0_ref, k1_ref, k2_ref, v0_ref, v1_ref, v2_ref, out_ref):
    c = pl.program_id(0)
    q = q_ref[0]
    rows = q.shape[0]
    scale = 1.0 / math.sqrt(AD)
    far = -1e30
    at_q = lax.broadcasted_iota(jnp.int32, (rows, rows), 0)
    at_k = lax.broadcasted_iota(jnp.int32, (rows, rows), 1)
    s0 = jnp.where(at_k <= at_q, times_t(q, k0_ref[0]) * scale, far)
    s1 = jnp.where(c >= early_ref[0], times_t(q, k1_ref[0]) * scale, far)
    s2 = jnp.where((at_k > at_q) & (c >= early_ref[1]), times_t(q, k2_ref[0]) * scale, far)
    top = jnp.max(jnp.maximum(jnp.maximum(s0, s1), s2), -1, keepdims=True)
    p0 = jnp.exp(s0 - top)
    p1 = jnp.exp(s1 - top)
    p2 = jnp.exp(s2 - top)
    denom = jnp.sum(p0 + p1 + p2, -1, keepdims=True)
    total = jnp.dot(p0.astype(jnp.bfloat16), v0_ref[0], preferred_element_type=jnp.float32)
    total += jnp.dot(p1.astype(jnp.bfloat16), v1_ref[0], preferred_element_type=jnp.float32)
    total += jnp.dot(p2.astype(jnp.bfloat16), v2_ref[0], preferred_element_type=jnp.float32)
    out_ref[0] = (total / denom).astype(out_ref.dtype)


def attend(early, q, keys, values):
    stretches, rows, width = q.shape
    block = (1, rows, AD)

    def own(c, h, early):
        return (c, 0, h)

    def behind(back):
        return lambda c, h, early: (jnp.maximum(c - early[back - 1], 0), 0, h)

    maps = [own, behind(1), behind(2)]
    specs = [pl.BlockSpec(block, m) for m in maps]
    return pl.pallas_call(
        attend_kernel,
        grid_spec=pltpu.PrefetchScalarGridSpec(
            num_scalar_prefetch=1,
            grid=(stretches, width // AD),
            in_specs=[pl.BlockSpec(block, own)] + specs + specs,
            out_specs=pl.BlockSpec(block, own),
        ),
        out_shape=jax.ShapeDtypeStruct(q.shape, jnp.bfloat16),
    )(early, q, *keys, *values)


def local(
    fast_query, fast_key, fast_value, rates, attn_query, attn_key, attn_value, fast_weights, gain
):
    stretches, rows, _ = fast_query.shape
    depth = fast_weights.shape[3]
    index = lax.axis_index(AA)
    first = lax.axis_index(PAIR) == 0
    parts = lax.axis_size(PLANE)

    def mine_and_other(a, b):
        return jnp.where(first, a, b), jnp.where(first, b, a)

    held = jnp.transpose(fast_weights.astype(jnp.bfloat16), (2, 1, 0, 3))
    mine, other = mine_and_other(held[0], held[1])
    chunk = jnp.concatenate([mine, partner(other)], 1)
    full = sent_to_all(chunk, PLANE)

    def swapped(x, c, size):
        a, b = mine_and_other(x[c, :, :size], x[c, :, size:])
        return jnp.concatenate([a, partner(b)], 0)

    keys = [swapped(fast_key, c, depth) for c in range(stretches)]
    values = [swapped(fast_value, c, depth) for c in range(stretches)]
    rate = [swapped(rates, c, 3) for c in range(stretches)]
    queries = [swapped(fast_query, c, depth) for c in range(stretches)]

    k1, v1 = from_behind(attn_key, AA, 1), from_behind(attn_value, AA, 1)
    k2, v2 = from_behind(attn_key, AA, 2), from_behind(attn_value, AA, 2)
    early = jnp.stack([index < 1, index < 2]).astype(jnp.int32)
    attention = attend(early, attn_query, (attn_key, k1, k2), (attn_value, v1, v2))

    def finish(out, c):
        back = partner(out[rows:].astype(jnp.bfloat16)).astype(jnp.float32)
        a, b = mine_and_other(out[:rows], back)
        combined = (jnp.concatenate([a, b], 1) + attention[c].astype(jnp.float32)).astype(
            jnp.bfloat16
        )
        size = lax.axis_size(BA)
        pieces = combined.reshape(size, rows // size, -1)
        got = lax.all_to_all(pieces, BA, split_axis=0, concat_axis=0, tiled=True)
        got = jnp.transpose(got, (1, 0, 2)).reshape(rows // size, -1).astype(jnp.float32)
        scale = lax.rsqrt(jnp.mean(got * got, -1, keepdims=True) + EPS)
        return (got * scale * gain).astype(jnp.bfloat16)

    wide = full.astype(jnp.float32)
    target = jnp.sqrt(jnp.sum(wide * wide, (0, 2)) + EPS)
    old = matrices(full)
    grads = summed_rows(gradient(*old, keys[0], values[0], rate[0], parts))
    out0 = answers(*old, queries[0])

    trial = wide - sent_to_all(grads.astype(jnp.bfloat16), PLANE).astype(jnp.float32)
    factor = target / jnp.sqrt(jnp.sum(trial * trial, (0, 2)) + EPS)
    new = matrices((trial * factor[None, :, None]).astype(jnp.bfloat16))
    own = (chunk.astype(jnp.float32) - grads) * factor[:, None]
    behind = grads * BETA
    local_rows = fast_weights.shape[0]
    own_other = partner(own[:, local_rows:])
    target_other = partner(target)

    moment = behind + summed_rows(gradient(*new, keys[1], values[1], rate[1], parts))
    out1 = answers(*new, queries[1])
    moment_other = partner(moment[:, local_rows:])
    last = own - moment
    squares = sent_to_all(jnp.sum(last * last, 1), AA)
    sides = [lax.axis_size(a) for a in AA]
    squares = jnp.sum(squares.reshape(*sides, 3, depth), (0, 2))
    squares, squares_other = mine_and_other(squares[0], squares[1])
    weights = last[:, :local_rows] * (target / jnp.sqrt(squares + EPS))[:, None]
    weights_other = (own_other - moment_other) * (
        target_other / jnp.sqrt(squares_other + EPS)
    )[:, None]

    def placed(a, b):
        return jnp.transpose(jnp.stack(mine_and_other(a, b)), (2, 1, 0, 3))

    mixed = jnp.stack([finish(out0, 0), finish(out1, 1)])
    return (
        mixed,
        placed(weights, weights_other),
        placed(moment[:, :local_rows], moment_other),
    )


def solution(mesh):
    torus = Mesh(mesh.devices.reshape(4, 2, 4, 2, 2), ("aa_0", "aa_1", "aa_2", "ba_0", "ba_1"))
    return jax.shard_map(
        local,
        mesh=torus,
        in_specs=(
            P(None, AA, BA),
            P(None, AA, BA),
            P(None, AA, BA),
            P(None, AA, BA),
            P(None, AA, BA),
            P(None, AA, BA),
            P(None, AA, BA),
            P(AA, None, BA, None),
            P(),
        ),
        out_specs=(P(None, AA_BA, None), P(AA, None, BA, None), P(AA, None, BA, None)),
        check_vma=False,
    )
```

```python
import math

import jax
import jax.numpy as jnp
from jax import lax
from jax.experimental import pallas as pl
from jax.experimental.pallas import tpu as pltpu
from jax.sharding import Mesh
from jax.sharding import PartitionSpec as P

AD = 128
AA = ("aa_0", "aa_1", "aa_2")
BA = ("ba_0", "ba_1")
AA_BA = ("aa_0", "aa_1", "aa_2", "ba_0", "ba_1")
PLANE = ("aa_0", "aa_2")
PAIR = "aa_1"

BETA = 0.9
EPS = 1e-06


def activation(x):
    sig = jax.nn.sigmoid(x)
    return (x * sig, sig * (1.0 + x * (1.0 - sig)))


def partner(x):
    return lax.ppermute(x, PAIR, [(0, 1), (1, 0)])


def sent_to_all(shard, axis):
    copies = jnp.broadcast_to(shard, (lax.axis_size(axis), *shard.shape))
    return lax.all_to_all(copies, axis, split_axis=0, concat_axis=0, tiled=True)


def gathered(chunk):
    row = sent_to_all(chunk, "aa_2")
    return sent_to_all(row, "aa_0").reshape(-1, *chunk.shape)


def after(x, done):
    zero = jnp.minimum(jnp.abs(done.reshape(-1)[-1].astype(jnp.float32)), 0.0)
    return x + zero.astype(x.dtype)


def from_behind(shard, axis, by):
    length = lax.axis_size(axis)
    return lax.ppermute(shard, axis, [(i, (i + by) % length) for i in range(length)])


def times_t(x, w):
    return lax.dot_general(x, w, (((1,), (1,)), ((), ())), preferred_element_type=jnp.float32)


def t_times(x, y):
    return lax.dot_general(x, y, (((0,), (0,)), ((), ())), preferred_element_type=jnp.float32)


def matrices(full):
    depth = full.shape[-1]
    return [full[:, i].reshape(-1, depth) for i in range(3)]


def answers(gate, up, down, q):
    act, _ = activation(times_t(q, gate))
    hidden = (act * times_t(q, up)).astype(jnp.bfloat16)
    return jnp.dot(hidden, down, preferred_element_type=jnp.float32)


def gradient(gate, up, down, k, v, rate, parts):
    gate_in = times_t(k, gate)
    up_in = times_t(k, up)
    back_in = times_t(v, down)
    act, slope = activation(gate_in)
    gate_x = (rate[:, 0:1] * (-back_in * up_in * slope)).astype(jnp.bfloat16)
    up_x = (rate[:, 1:2] * (-back_in * act)).astype(jnp.bfloat16)
    down_x = (rate[:, 2:3] * -(act * up_in)).astype(jnp.bfloat16)
    terms = [t_times(gate_x, k), t_times(up_x, k), t_times(down_x, v)]
    return jnp.stack(
        [t.astype(jnp.bfloat16).reshape(parts, -1, t.shape[-1]) for t in terms], 1
    )


def summed_rows(terms):
    side = lax.axis_size("aa_0")
    terms = terms.reshape(side, -1, *terms.shape[1:])
    got = lax.all_to_all(terms, "aa_0", split_axis=0, concat_axis=0, tiled=True)
    rows = jnp.sum(got.astype(jnp.float32), 0).astype(jnp.bfloat16)
    got = lax.all_to_all(rows, "aa_2", split_axis=0, concat_axis=0, tiled=True)
    return jnp.sum(got.astype(jnp.float32), 0)


def attend_kernel(early_ref, q_ref, k0_ref, k1_ref, k2_ref, v0_ref, v1_ref, v2_ref, out_ref):
    c = pl.program_id(0)
    q = q_ref[0]
    rows = q.shape[0]
    scale = 1.0 / math.sqrt(AD)
    far = -1e30
    at_q = lax.broadcasted_iota(jnp.int32, (rows, rows), 0)
    at_k = lax.broadcasted_iota(jnp.int32, (rows, rows), 1)
    s0 = jnp.where(at_k <= at_q, times_t(q, k0_ref[0]) * scale, far)
    s1 = jnp.where(c >= early_ref[0], times_t(q, k1_ref[0]) * scale, far)
    s2 = jnp.where((at_k > at_q) & (c >= early_ref[1]), times_t(q, k2_ref[0]) * scale, far)
    top = jnp.max(jnp.maximum(jnp.maximum(s0, s1), s2), -1, keepdims=True)
    p0 = jnp.exp(s0 - top)
    p1 = jnp.exp(s1 - top)
    p2 = jnp.exp(s2 - top)
    denom = jnp.sum(p0 + p1 + p2, -1, keepdims=True)
    total = jnp.dot(p0.astype(jnp.bfloat16), v0_ref[0], preferred_element_type=jnp.float32)
    total += jnp.dot(p1.astype(jnp.bfloat16), v1_ref[0], preferred_element_type=jnp.float32)
    total += jnp.dot(p2.astype(jnp.bfloat16), v2_ref[0], preferred_element_type=jnp.float32)
    out_ref[0] = (total / denom).astype(out_ref.dtype)


def attend(early, q, keys, values):
    stretches, rows, width = q.shape
    block = (1, rows, AD)

    def own(c, h, early):
        return (c, 0, h)

    def behind(back):
        return lambda c, h, early: (jnp.maximum(c - early[back - 1], 0), 0, h)

    maps = [own, behind(1), behind(2)]
    specs = [pl.BlockSpec(block, m) for m in maps]
    return pl.pallas_call(
        attend_kernel,
        grid_spec=pltpu.PrefetchScalarGridSpec(
            num_scalar_prefetch=1,
            grid=(stretches, width // AD),
            in_specs=[pl.BlockSpec(block, own)] + specs + specs,
            out_specs=pl.BlockSpec(block, own),
        ),
        out_shape=jax.ShapeDtypeStruct(q.shape, jnp.bfloat16),
    )(early, q, *keys, *values)


def step(
    fast_query, fast_key, fast_value, rates, attn_query, attn_key, attn_value, fast_weights, gain
):
    stretches, rows, _ = fast_query.shape
    depth = fast_weights.shape[3]
    index = lax.axis_index(AA)
    first = lax.axis_index(PAIR) == 0
    parts = lax.axis_size(PLANE)

    def mine_and_other(a, b):
        return jnp.where(first, a, b), jnp.where(first, b, a)

    held = jnp.transpose(fast_weights.astype(jnp.bfloat16), (2, 1, 0, 3))
    mine, other = mine_and_other(held[0], held[1])
    chunk = jnp.concatenate([mine, partner(other)], 1)
    full = gathered(chunk)

    def swapped(x, c, size):
        a, b = mine_and_other(x[c, :, :size], x[c, :, size:])
        return jnp.concatenate([a, partner(b)], 0)

    rate = [swapped(rates, c, 3) for c in range(stretches)]
    key0, value0 = swapped(fast_key, 0, depth), swapped(fast_value, 0, depth)
    key1, value1 = swapped(fast_key, 1, depth), swapped(fast_value, 1, depth)
    query0, query1 = swapped(fast_query, 0, depth), swapped(fast_query, 1, depth)
    sent_key, sent_value = after(attn_key, key1), after(attn_value, value1)
    k1, v1 = from_behind(sent_key, AA, 1), from_behind(sent_value, AA, 1)
    k2, v2 = from_behind(sent_key, AA, 2), from_behind(sent_value, AA, 2)

    def finish(outs, attention):
        back = partner(jnp.stack([o[rows:] for o in outs]).astype(jnp.bfloat16))
        a, b = mine_and_other(jnp.stack([o[:rows] for o in outs]), back.astype(jnp.float32))
        combined = (jnp.concatenate([a, b], 2) + attention.astype(jnp.float32)).astype(
            jnp.bfloat16
        )
        size = lax.axis_size(BA)
        pieces = jnp.moveaxis(combined.reshape(stretches, size, rows // size, -1), 1, 0)
        got = lax.all_to_all(pieces, BA, split_axis=0, concat_axis=0, tiled=True)
        got = jnp.transpose(got, (1, 2, 0, 3)).reshape(stretches, rows // size, -1)
        got = got.astype(jnp.float32)
        scale = lax.rsqrt(jnp.mean(got * got, -1, keepdims=True) + EPS)
        return (got * scale * gain).astype(jnp.bfloat16)

    wide = full.astype(jnp.float32)
    target = jnp.sqrt(jnp.sum(wide * wide, (0, 2)) + EPS)
    old = matrices(full)
    terms = gradient(*old, key0, value0, rate[0], parts)
    grads = summed_rows(terms)

    trial = wide - gathered(grads.astype(jnp.bfloat16)).astype(jnp.float32)
    factor = target / jnp.sqrt(jnp.sum(trial * trial, (0, 2)) + EPS)
    new = matrices((trial * factor[None, :, None]).astype(jnp.bfloat16))
    own = (chunk.astype(jnp.float32) - grads) * factor[:, None]
    behind = grads * BETA
    local_rows = fast_weights.shape[0]
    own_other = partner(own[:, local_rows:])
    target_other = partner(target)

    terms = gradient(*new, key1, value1, rate[1], parts)
    moment = behind + summed_rows(terms)
    out0 = answers(*old, after(query0, terms))
    out1 = answers(*new, after(query1, terms))
    early = after(jnp.stack([index < 1, index < 2]).astype(jnp.int32), terms)
    attention = attend(early, attn_query, (attn_key, k1, k2), (attn_value, v1, v2))
    moment_other = partner(moment[:, local_rows:])
    last = own - moment
    squares = sent_to_all(jnp.sum(last * last, 1), AA)
    sides = [lax.axis_size(a) for a in AA]
    squares = jnp.sum(squares.reshape(*sides, 3, depth), (0, 2))
    squares, squares_other = mine_and_other(squares[0], squares[1])
    weights = last[:, :local_rows] * (target / jnp.sqrt(squares + EPS))[:, None]
    weights_other = (own_other - moment_other) * (
        target_other / jnp.sqrt(squares_other + EPS)
    )[:, None]

    def placed(a, b):
        return jnp.transpose(jnp.stack(mine_and_other(a, b)), (2, 1, 0, 3))

    mixed = finish([out0, out1], attention)
    return (
        mixed,
        placed(weights, weights_other),
        placed(moment[:, :local_rows], moment_other),
    )


def solution(mesh):
    torus = Mesh(mesh.devices.reshape(4, 2, 4, 2, 2), ("aa_0", "aa_1", "aa_2", "ba_0", "ba_1"))
    return jax.shard_map(
        step,
        mesh=torus,
        in_specs=(
            P(None, AA, BA),
            P(None, AA, BA),
            P(None, AA, BA),
            P(None, AA, BA),
            P(None, AA, BA),
            P(None, AA, BA),
            P(None, AA, BA),
            P(AA, None, BA, None),
            P(),
        ),
        out_specs=(P(None, AA_BA, None), P(AA, None, BA, None), P(AA, None, BA, None)),
        check_vma=False,
    )
```

```python
import math

import jax
import jax.numpy as jnp
from jax import lax
from jax.experimental import pallas as pl
from jax.experimental.pallas import tpu as pltpu
from jax.sharding import Mesh
from jax.sharding import PartitionSpec as P

AD = 128
AA = ("aa_0", "aa_1", "aa_2")
BA = ("ba_0", "ba_1")
AA_BA = ("aa_0", "aa_1", "aa_2", "ba_0", "ba_1")
PLANE = ("aa_0", "aa_2")
PAIR = "aa_1"

BETA = 0.9
EPS = 1e-06


def activation(x):
    sig = jax.nn.sigmoid(x)
    return (x * sig, sig * (1.0 + x * (1.0 - sig)))


def partner(x):
    return lax.ppermute(x, PAIR, [(0, 1), (1, 0)])


def sent_to_all(shard, axis):
    copies = jnp.broadcast_to(shard, (lax.axis_size(axis), *shard.shape))
    return lax.all_to_all(copies, axis, split_axis=0, concat_axis=0, tiled=True)


def gathered_row(chunk):
    return sent_to_all(chunk, "aa_2")


def gathered(row):
    return sent_to_all(row, "aa_0").reshape(-1, *row.shape[1:])


def after(x, done):
    zero = jnp.minimum(jnp.abs(done.reshape(-1)[-1].astype(jnp.float32)), 0.0)
    return x + zero.astype(x.dtype)


def from_behind(shard, axis, by):
    length = lax.axis_size(axis)
    return lax.ppermute(shard, axis, [(i, (i + by) % length) for i in range(length)])


def times_t(x, w):
    return lax.dot_general(x, w, (((1,), (1,)), ((), ())), preferred_element_type=jnp.float32)


def t_times(x, y):
    return lax.dot_general(x, y, (((0,), (0,)), ((), ())), preferred_element_type=jnp.float32)


def matrices(full):
    depth = full.shape[-1]
    return [full[:, i].reshape(-1, depth) for i in range(3)]


def answers(gate, up, down, q):
    act, _ = activation(times_t(q, gate))
    hidden = (act * times_t(q, up)).astype(jnp.bfloat16)
    return jnp.dot(hidden, down, preferred_element_type=jnp.float32)


def gradient(gate, up, down, k, v, rate, parts):
    gate_in = times_t(k, gate)
    up_in = times_t(k, up)
    back_in = times_t(v, down)
    act, slope = activation(gate_in)
    gate_x = (rate[:, 0:1] * (-back_in * up_in * slope)).astype(jnp.bfloat16)
    up_x = (rate[:, 1:2] * (-back_in * act)).astype(jnp.bfloat16)
    down_x = (rate[:, 2:3] * -(act * up_in)).astype(jnp.bfloat16)
    terms = [t_times(gate_x, k), t_times(up_x, k), t_times(down_x, v)]
    return jnp.stack(
        [t.astype(jnp.bfloat16).reshape(parts, -1, t.shape[-1]) for t in terms], 1
    )


def summed_rows(terms, *done):
    side = lax.axis_size("aa_0")
    terms = terms.reshape(side, -1, *terms.shape[1:])
    got = lax.all_to_all(terms, "aa_0", split_axis=0, concat_axis=0, tiled=True)
    rows = jnp.sum(got.astype(jnp.float32), 0).astype(jnp.bfloat16)
    for d in done:
        rows = after(rows, d)
    got = lax.all_to_all(rows, "aa_2", split_axis=0, concat_axis=0, tiled=True)
    return jnp.sum(got.astype(jnp.float32), 0)


def attend_kernel(early_ref, q_ref, k0_ref, k1_ref, k2_ref, v0_ref, v1_ref, v2_ref, out_ref):
    c = pl.program_id(0)
    q = q_ref[0]
    rows = q.shape[0]
    scale = 1.0 / math.sqrt(AD)
    far = -1e30
    at_q = lax.broadcasted_iota(jnp.int32, (rows, rows), 0)
    at_k = lax.broadcasted_iota(jnp.int32, (rows, rows), 1)
    s0 = jnp.where(at_k <= at_q, times_t(q, k0_ref[0]) * scale, far)
    s1 = jnp.where(c >= early_ref[0], times_t(q, k1_ref[0]) * scale, far)
    s2 = jnp.where((at_k > at_q) & (c >= early_ref[1]), times_t(q, k2_ref[0]) * scale, far)
    top = jnp.max(jnp.maximum(jnp.maximum(s0, s1), s2), -1, keepdims=True)
    p0 = jnp.exp(s0 - top)
    p1 = jnp.exp(s1 - top)
    p2 = jnp.exp(s2 - top)
    denom = jnp.sum(p0 + p1 + p2, -1, keepdims=True)
    total = jnp.dot(p0.astype(jnp.bfloat16), v0_ref[0], preferred_element_type=jnp.float32)
    total += jnp.dot(p1.astype(jnp.bfloat16), v1_ref[0], preferred_element_type=jnp.float32)
    total += jnp.dot(p2.astype(jnp.bfloat16), v2_ref[0], preferred_element_type=jnp.float32)
    out_ref[0] = (total / denom).astype(out_ref.dtype)


def attend(early, q, keys, values):
    stretches, rows, width = q.shape
    block = (1, rows, AD)

    def own(c, h, early):
        return (c, 0, h)

    def behind(back):
        return lambda c, h, early: (jnp.maximum(c - early[back - 1], 0), 0, h)

    maps = [own, behind(1), behind(2)]
    specs = [pl.BlockSpec(block, m) for m in maps]
    return pl.pallas_call(
        attend_kernel,
        grid_spec=pltpu.PrefetchScalarGridSpec(
            num_scalar_prefetch=1,
            grid=(stretches, width // AD),
            in_specs=[pl.BlockSpec(block, own)] + specs + specs,
            out_specs=pl.BlockSpec(block, own),
        ),
        out_shape=jax.ShapeDtypeStruct(q.shape, jnp.bfloat16),
    )(early, q, *keys, *values)


def step(
    fast_query, fast_key, fast_value, rates, attn_query, attn_key, attn_value, fast_weights, gain
):
    stretches, rows, _ = fast_query.shape
    depth = fast_weights.shape[3]
    index = lax.axis_index(AA)
    first = lax.axis_index(PAIR) == 0
    parts = lax.axis_size(PLANE)

    def mine_and_other(a, b):
        return jnp.where(first, a, b), jnp.where(first, b, a)

    held = jnp.transpose(fast_weights.astype(jnp.bfloat16), (2, 1, 0, 3))
    mine, other = mine_and_other(held[0], held[1])
    chunk = jnp.concatenate([mine, partner(other)], 1)
    full = gathered(gathered_row(chunk))

    def swapped(x, c, size):
        a, b = mine_and_other(x[c, :, :size], x[c, :, size:])
        return jnp.concatenate([a, partner(b)], 0)

    rate = [swapped(rates, c, 3) for c in range(stretches)]
    key0, value0 = swapped(fast_key, 0, depth), swapped(fast_value, 0, depth)
    key1, value1 = swapped(fast_key, 1, depth), swapped(fast_value, 1, depth)
    sent_key, sent_value = after(attn_key, key1), after(attn_value, value1)
    k1, v1 = from_behind(sent_key, AA, 1), from_behind(sent_value, AA, 1)

    def finish(outs, attention):
        back = partner(jnp.stack([o[rows:] for o in outs]).astype(jnp.bfloat16))
        a, b = mine_and_other(jnp.stack([o[:rows] for o in outs]), back.astype(jnp.float32))
        combined = (jnp.concatenate([a, b], 2) + attention.astype(jnp.float32)).astype(
            jnp.bfloat16
        )
        size = lax.axis_size(BA)
        pieces = jnp.moveaxis(combined.reshape(stretches, size, rows // size, -1), 1, 0)
        got = lax.all_to_all(pieces, BA, split_axis=0, concat_axis=0, tiled=True)
        got = jnp.transpose(got, (1, 2, 0, 3)).reshape(stretches, rows // size, -1)
        got = got.astype(jnp.float32)
        scale = lax.rsqrt(jnp.mean(got * got, -1, keepdims=True) + EPS)
        return (got * scale * gain).astype(jnp.bfloat16)

    wide = full.astype(jnp.float32)
    target = jnp.sqrt(jnp.sum(wide * wide, (0, 2)) + EPS)
    old = matrices(full)
    terms = gradient(*old, key0, value0, rate[0], parts)
    grads = summed_rows(terms, k1, v1)
    row = gathered_row(grads.astype(jnp.bfloat16))
    sent_key, sent_value = after(k1, row), after(v1, row)
    k2, v2 = from_behind(sent_key, AA, 1), from_behind(sent_value, AA, 1)
    change = gathered(row)
    queries = after(fast_query, v1)
    query0, query1 = swapped(queries, 0, depth), swapped(queries, 1, depth)

    trial = wide - change.astype(jnp.float32)
    factor = target / jnp.sqrt(jnp.sum(trial * trial, (0, 2)) + EPS)
    new = matrices((trial * factor[None, :, None]).astype(jnp.bfloat16))
    own = (chunk.astype(jnp.float32) - grads) * factor[:, None]
    behind = grads * BETA
    local_rows = fast_weights.shape[0]
    own_other = partner(own[:, local_rows:])
    target_other = partner(target)

    terms = gradient(*new, key1, value1, rate[1], parts)
    moment = behind + summed_rows(terms)
    out0 = answers(*old, after(query0, terms))
    out1 = answers(*new, after(query1, terms))
    early = after(jnp.stack([index < 1, index < 2]).astype(jnp.int32), terms)
    attention = attend(early, attn_query, (attn_key, k1, k2), (attn_value, v1, v2))
    moment_other = partner(moment[:, local_rows:])
    last = own - moment
    squares = sent_to_all(jnp.sum(last * last, 1), AA)
    sides = [lax.axis_size(a) for a in AA]
    squares = jnp.sum(squares.reshape(*sides, 3, depth), (0, 2))
    squares, squares_other = mine_and_other(squares[0], squares[1])
    weights = last[:, :local_rows] * (target / jnp.sqrt(squares + EPS))[:, None]
    weights_other = (own_other - moment_other) * (
        target_other / jnp.sqrt(squares_other + EPS)
    )[:, None]

    def placed(a, b):
        return jnp.transpose(jnp.stack(mine_and_other(a, b)), (2, 1, 0, 3))

    mixed = finish([out0, out1], attention)
    return (
        mixed,
        placed(weights, weights_other),
        placed(moment[:, :local_rows], moment_other),
    )


def solution(mesh):
    torus = Mesh(mesh.devices.reshape(4, 2, 4, 2, 2), ("aa_0", "aa_1", "aa_2", "ba_0", "ba_1"))
    return jax.shard_map(
        step,
        mesh=torus,
        in_specs=(
            P(None, AA, BA),
            P(None, AA, BA),
            P(None, AA, BA),
            P(None, AA, BA),
            P(None, AA, BA),
            P(None, AA, BA),
            P(None, AA, BA),
            P(AA, None, BA, None),
            P(),
        ),
        out_specs=(P(None, AA_BA, None), P(AA, None, BA, None), P(AA, None, BA, None)),
        check_vma=False,
    )
```
